256 devices in a mesh: batch: 4 (over z_lo), grid: 64 (over x, y, z_hi, core).
Axes of the slice: x: 4, y: 4, z: 8 (z_hi: 2, z_lo: 4; z = z_hi * 4 + z_lo), core: 2. Of those that a mesh axis runs over, the one named last changes fastest.
Arguments:
- fields: bfloat16 [1024, 512, 512], P(('batch', 'grid')), parts along dimension 0, may hold values from -18 to 18
- norm_gain: float32 [256], replicated, may hold values from 0.5 to 1.5
- norm_shift: float32 [256], replicated, may hold values from -3 to 3
- first_weight: bfloat16 [2, 8, 32, 32], replicated, may hold values from -0.75 to 0.75
- second_weight: bfloat16 [2, 8, 32, 32], replicated, may hold values from -0.75 to 0.75
- first_bias: float32 [2, 256], replicated, may hold values from -2 to 2
Outputs:
- mixed_fields: bfloat16 [1024, 512, 512], P(('batch', 'grid')), parts along dimension 0
The draws below stay inside these ranges and needn't reach their ends.
There are 4 independent parts, one for each index of `batch`. The reference program is written for one: setup_inputs(seed, part) draws one part's arguments, and reference() takes and returns one part's arrays. A program takes and returns all parts, laid end to end along the dimension named above; an argument that names none is the same for every part. Nothing has to cross between parts.
All inputs are finite; a program needn't handle non-finite values.
Results may differ from the reference program's by a relative error of at most 0.0055.
Values may be sent and summed in bfloat16 or wider, within the bound.
A program may use at most 64 MiB of HBM per device.

```python
import math
import jax
import jax.numpy as jnp
from jax import lax

C = 256
BS = 32
H = 512
W = 512
NB = 8


def draw_fields(key, part):
    first_key = jax.random.fold_in(key, 11)
    ramp = jnp.arange(C, dtype=jnp.float32) / (C - 1)
    base = jnp.clip(jax.random.normal(first_key, (C, H, W), jnp.float32), -4.0, 4.0)
    scale = jnp.power(3.0, ramp)
    return (base * scale[:, None, None]).astype(jnp.bfloat16)


def normal_values(key, extent, scale, bound, kind=jnp.bfloat16):
    entries = scale * jax.random.normal(key, extent, jnp.float32)
    return jnp.clip(entries, min=-bound, max=bound).astype(kind)


def setup_inputs(seed: int = 0, part: int = 0) -> dict:
    splits = jax.random.split(jax.random.key(seed), 7)
    part_splits = jax.random.split(jax.random.fold_in(splits[6], part), 7)
    return {
        "fields": draw_fields(jax.random.fold_in(jax.random.fold_in(splits[6], part), 71), part),
        "norm_gain": jnp.clip(1.0 + 0.1 * jax.random.normal(splits[1], (C,), jnp.float32), 0.5, 1.5),
        "norm_shift": normal_values(splits[2], (C,), 0.5, 3.0, jnp.float32),
        "first_weight": normal_values(splits[3], (2, NB, BS, BS), (2 * BS) ** -0.5, 0.75),
        "second_weight": normal_values(splits[4], (2, NB, BS, BS), (2 * BS) ** -0.5, 0.75),
        "first_bias": normal_values(splits[5], (2, C), 0.3, 2.0, jnp.float32),
    }


def tables(rows, cols):
    half = cols // 2
    col_index = jnp.arange(cols, dtype=jnp.int32)
    mode_index = jnp.arange(half, dtype=jnp.int32)
    angle_w = (col_index[:, None] * mode_index[None, :] % cols).astype(jnp.float32) * (2.0 * math.pi / cols)
    scale_w = 1.0 / math.sqrt(cols)
    fwd_w = jnp.concatenate([jnp.cos(angle_w) * scale_w, -jnp.sin(angle_w) * scale_w], axis=1).astype(jnp.bfloat16)
    weight_k = jnp.where(mode_index == 0, 1.0, 2.0).astype(jnp.float32)
    inv_w = jnp.concatenate([(jnp.cos(angle_w) * weight_k[None, :] * scale_w).T, (-jnp.sin(angle_w) * weight_k[None, :] * scale_w).T], axis=0).astype(jnp.bfloat16)
    row_index = jnp.arange(rows, dtype=jnp.int32)
    angle_h = (row_index[:, None] * row_index[None, :] % rows).astype(jnp.float32) * (2.0 * math.pi / rows)
    scale_h = 1.0 / math.sqrt(rows)
    cos_h = (jnp.cos(angle_h) * scale_h).astype(jnp.bfloat16)
    sin_h = (jnp.sin(angle_h) * scale_h).astype(jnp.bfloat16)
    return (fwd_w, inv_w, cos_h, sin_h)

def mult(form, left, right):
    return jnp.einsum(form, left.astype(jnp.float32), right.astype(jnp.float32), precision=lax.Precision.HIGHEST)

def shrink(values):
    return jnp.maximum(values - 0.01, 0.0) + jnp.minimum(values + 0.01, 0.0)

def mix_modes(real_part, imag_part, first_weight, second_weight, first_bias):
    blocks = first_weight.shape[1]
    width = first_weight.shape[2]
    shape = real_part.shape
    real_blk = real_part.reshape(blocks, width, -1)
    imag_blk = imag_part.reshape(blocks, width, -1)
    bias_blk = first_bias.reshape(2, blocks, width, 1)
    hid_re = jax.nn.relu(mult('bio,bim->bom', first_weight[0], real_blk) - mult('bio,bim->bom', first_weight[1], imag_blk) + bias_blk[0]).astype(jnp.bfloat16)
    hid_im = jax.nn.relu(mult('bio,bim->bom', first_weight[0], imag_blk) + mult('bio,bim->bom', first_weight[1], real_blk) + bias_blk[1]).astype(jnp.bfloat16)
    out_re = mult('bio,bim->bom', second_weight[0], hid_re) - mult('bio,bim->bom', second_weight[1], hid_im)
    out_im = mult('bio,bim->bom', second_weight[0], hid_im) + mult('bio,bim->bom', second_weight[1], hid_re)
    return (shrink(out_re).astype(jnp.bfloat16).reshape(shape), shrink(out_im).astype(jnp.bfloat16).reshape(shape))

def reference(fields, norm_gain, norm_shift, first_weight, second_weight, first_bias):
    channels, rows, cols = fields.shape
    half = cols // 2
    fwd_w, inv_w, cos_h, sin_h = tables(rows, cols)
    values = fields.astype(jnp.float32)
    mean = lax.optimization_barrier(jnp.mean(values, axis=0))
    mean_sq = lax.optimization_barrier(jnp.mean(values * values, axis=0))
    var = mean_sq - mean * mean
    normed = ((values - mean) * lax.rsqrt(var + 1e-05) * norm_gain[:, None, None] + norm_shift[:, None, None]).astype(jnp.bfloat16)
    along_w = mult('chw,wk->chk', normed, fwd_w).astype(jnp.bfloat16).reshape(channels, rows, 2, half)
    first_p = mult('kh,chpq->ckpq', cos_h, along_w)
    first_q = mult('kh,chpq->ckpq', sin_h, along_w)
    modes_re = (first_p[:, :, 0] + first_q[:, :, 1]).astype(jnp.bfloat16)
    modes_im = (first_p[:, :, 1] - first_q[:, :, 0]).astype(jnp.bfloat16)
    shr_re, shr_im = mix_modes(modes_re, modes_im, first_weight, second_weight, first_bias)
    shrunk = jnp.stack([shr_re, shr_im], axis=2)
    back_p = mult('kh,ckpq->chpq', cos_h, shrunk)
    back_q = mult('kh,ckpq->chpq', sin_h, shrunk)
    back_re = (back_p[:, :, 0] - back_q[:, :, 1]).astype(jnp.bfloat16)
    back_im = (back_p[:, :, 1] + back_q[:, :, 0]).astype(jnp.bfloat16)
    backed = jnp.concatenate([back_re, back_im], axis=2)
    filtered = mult('chk,kw->chw', backed, inv_w)
    return (values + filtered).astype(jnp.bfloat16)
```

```python
import functools
import math

import jax
import jax.numpy as jnp
import ml_dtypes
import numpy as np
from jax import lax
from jax.experimental import pallas as pl
from jax.experimental.pallas import tpu as pltpu
from jax.sharding import PartitionSpec as P

MESH = pl.DeviceIdType.MESH
BF = jnp.bfloat16
F32 = jnp.float32
N = 512
ROWS = 128
RS = 40
SS = 520
KB = 16


def tables():
    half = N // 2
    idx = np.arange(N)
    step = np.float32(2.0 * math.pi / N)
    scale = np.float32(1.0 / math.sqrt(N))
    angle_w = ((idx[:, None] * np.arange(half)[None, :]) % N).astype(np.float32) * step
    cos_w, sin_w = np.cos(angle_w), np.sin(angle_w)
    weight = np.where(np.arange(half) == 0, 1.0, 2.0).astype(np.float32)
    re, im = cos_w * scale, -sin_w * scale
    fwd = np.stack(
        [np.concatenate([re[:, s], im[:, s]], 1) for s in (slice(0, 128), slice(128, 256))]
    )
    ire, iim = (cos_w * weight * scale).T, (-sin_w * weight * scale).T
    inv = np.stack(
        [np.concatenate([ire[s], iim[s]], 0) for s in (slice(0, 128), slice(128, 256))]
    )
    angle_h = ((idx[:, None] * idx[None, :]) % N).astype(np.float32) * step
    both = np.concatenate([np.cos(angle_h) * scale, np.sin(angle_h) * scale], 1)
    cast = lambda a: a.astype(ml_dtypes.bfloat16)
    return cast(fwd), cast(inv), cast(both)


def kernel(
    f_hbm, gain, shift, w1, w2, bias, fwd_hbm, inv_hbm, both_hbm,
    out_hbm,
    fld, mode_re, mode_im, shr_re, shr_im, stat, part, xbuf, xsum, ybuf, ysum, zbuf,
    fwd_t, inv_t, both_t, big1, big2, bcol, stack, back_own, back_out, back_in, out_v,
    zs, zr, ys, yr, ds, dr, os, orr, cys, cyr, czs, czr, cds, cdr,
    xs1, xr1, ys1, yr1, zs1, zr1, ys2, yr2, xs2, xr2, cs2, cr2, bs, br, loc, tab, outs,
):
    b = lax.axis_index("batch")
    g = lax.axis_index("grid")
    core = lax.rem(g, 2)
    zh = lax.rem(lax.div(g, 2), 2)
    y = lax.rem(lax.div(g, 4), 4)
    x = lax.div(g, 16)
    yy = lax.rem(y, 2)
    blk = lax.div(g, 8)

    def dev(x_, y_, z_, c_):
        return (b, ((x_ * 4 + y_) * 2 + z_) * 2 + c_)

    def flip(v, d):
        return v + d - 2 * v * d

    def base(dy, dz, dc):
        return ((flip(yy, dy) * 2 + flip(zh, dz)) * 2 + flip(core, dc)) * 4

    ypart = dev(x, y + 1 - 2 * yy, zh, core)
    zpart = dev(x, y, 1 - zh, core)
    cpart = dev(x, y, zh, 1 - core)
    xpeer = [lax.rem(x + 4 - d, 4) for d in (1, 2, 3)]
    ypeer = [lax.rem(y + 4 - d, 4) for d in (1, 2, 3)]
    xdev = [dev(v, y, zh, core) for v in xpeer]
    ydev = [dev(x, v, zh, core) for v in ypeer]

    def remote(src, dst, send, recv, to):
        return pltpu.make_async_remote_copy(
            src_ref=src, dst_ref=dst, send_sem=send, recv_sem=recv, device_id=to, device_id_type=MESH
        )

    own = base(0, 0, 0)
    tabs = [
        pltpu.make_async_copy(fwd_hbm.at[core], fwd_t, tab.at[0]),
        pltpu.make_async_copy(inv_hbm, inv_t, tab.at[1]),
        pltpu.make_async_copy(both_hbm, both_t, tab.at[2]),
    ]
    fetch = [pltpu.make_async_copy(f_hbm.at[i], fld.at[own + i], loc.at[i]) for i in range(4)]
    for c in fetch:
        c.start()

    barrier = pltpu.get_barrier_semaphore()
    peers = xdev + ydev + [zpart, cpart]
    for p in peers:
        pl.semaphore_signal(barrier, inc=1, device_id=p, device_id_type=MESH)
    pl.semaphore_wait(barrier, len(peers))
    for c in fetch:
        c.wait()
    for c in tabs:
        c.start()

    def piece(first, n):
        row = pl.multiple_of((n % 4) * ROWS, ROWS)
        return fld.at[first + n // 4, pl.ds(row, ROWS), :]

    def same(ref, send, recv, to):
        return remote(ref, ref, send, recv, to)

    def zchunk(n):
        return same(piece(own, n), zs.at[0], zr.at[n], zpart)

    def ychunk(n):
        return same(piece(own, n), ys.at[0], yr.at[n], ypart)

    def dchunk(n):
        return same(piece(base(0, 1, 0), n), ds.at[0], dr.at[n], ypart)

    def cychunk(n):
        return same(piece(base(1, 0, 0), n), cys.at[0], cyr.at[n], cpart)

    def czchunk(n):
        return same(piece(base(0, 1, 0), n), czs.at[0], czr.at[n], cpart)

    def cdchunk(n):
        return same(piece(base(1, 1, 0), n), cds.at[0], cdr.at[n], cpart)

    def owncopy(i, h):
        rows = pl.ds(pl.multiple_of(256 * h, 256), 256)
        return fld.at[own + i, rows, :]

    ownc = [same(owncopy(i, 1 - core), os.at[0], orr.at[i], cpart) for i in range(4)]
    ownc += [same(owncopy(i, core), os.at[0], orr.at[4 + i], cpart) for i in range(4)]
    for c in ownc[:4]:
        c.start()
    for n in range(3):
        zchunk(n).start()
    for n in range(5):
        ychunk(n).start()
    for c in ownc[4:]:
        c.start()

    for c in ownc[:4]:
        c.wait_recv()
    other = base(0, 0, 1)

    def partial_sums(r, _):
        row = pl.multiple_of(256 * core + r * 16, 16)
        s1 = jnp.zeros((16, N), F32)
        s2 = jnp.zeros((16, N), F32)
        for first in (own, other):
            for i in range(4):
                v = fld[first + i, pl.ds(row, 16), :].astype(F32)
                s1 = s1 + v
                s2 = s2 + v * v
        at = pl.ds(pl.multiple_of(r * 16, 16), 16)
        part[0, at, :] = s1
        part[1, at, :] = s2
        return 0

    lax.fori_loop(0, 16, partial_sums, 0)

    xrs = [
        remote(
            part.at[:, pl.ds(pl.multiple_of(64 * xpeer[d], 64), 64), :],
            xbuf.at[d], xs1.at[d], xr1.at[d], xdev[d],
        )
        for d in range(3)
    ]
    for c in xrs:
        c.start()

    for c in tabs:
        c.wait()

    def iota(shape, dim):
        return lax.broadcasted_iota(jnp.int32, shape, dim)

    pick = (iota((256, 32), 0) % 32 == iota((256, 32), 1)).astype(BF)
    nt = (((1,), (1,)), ((), ()))

    def expand(rows, w, sel):
        left = lax.dot_general(sel, w, nt, preferred_element_type=F32).astype(BF)
        return lax.dot_general(left, pick, nt, preferred_element_type=F32)

    def complex_matrix(rows, per, sel, w):
        t0 = expand(rows, w[0, blk], sel)
        t1 = expand(rows, w[1, blk], sel)
        r = iota((rows, 256), 0)
        c = iota((rows, 256), 1)
        rp, cp = r // (4 * per), c // 128
        hit = (r // per) % 4 == (c // 32) % 4
        val = jnp.where(rp == cp, t0, jnp.where(rp == 1, t1, -t1))
        return jnp.where(hit, val, 0.0).astype(BF)

    big1[...] = complex_matrix(256, 32, pick, w1)
    chip = yy * 2 + zh
    pick2 = ((iota((64, 32), 0) % 8) + chip * 8 == iota((64, 32), 1)).astype(BF)
    big2[...] = complex_matrix(64, 8, pick2, w2)
    r = iota((256, 256), 0)
    c = iota((256, 256), 1)
    hit = (r % 32) + blk * 32 == c
    value = jnp.where(r < 128, bias[0:1, :], bias[1:2, :])
    col = jnp.sum(jnp.where(hit, value, 0.0), axis=1, keepdims=True)
    bcol[...] = jnp.broadcast_to(col, (256, 128))

    for c in xrs:
        c.wait_recv()
    mine = pl.ds(pl.multiple_of(64 * x, 64), 64)
    xsum[...] = part[:, mine, :] + xbuf[0] + xbuf[1] + xbuf[2]
    yrs = [
        remote(
            xsum.at[:, pl.ds(pl.multiple_of(16 * ypeer[d], 16), 16), :],
            ybuf.at[d], ys1.at[d], yr1.at[d], ydev[d],
        )
        for d in range(3)
    ]
    for c in yrs:
        c.start()
    for n in range(5, 8):
        ychunk(n).start()
    for c in yrs:
        c.wait_recv()
    mine = pl.ds(pl.multiple_of(16 * y, 16), 16)
    ysum[...] = xsum[:, mine, :] + ybuf[0] + ybuf[1] + ybuf[2]
    zex = remote(ysum, zbuf, zs1.at[0], zr1.at[0], zpart)
    zex.start()
    for n in range(3, 16):
        zchunk(n).start()
    zex.wait_recv()
    total = ysum[...] + zbuf[...]
    mean = total[0] * (1.0 / 256.0)
    var = total[1] * (1.0 / 256.0) - mean * mean
    row0 = 256 * core + 64 * x
    mine = pl.ds(pl.multiple_of(row0 + 16 * y, 16), 16)
    stat[0, mine, :] = mean
    stat[1, mine, :] = lax.rsqrt(var + 1e-5)
    yag = [same(stat.at[:, mine, :], ys2.at[d], yr2.at[d], ydev[d]) for d in range(3)]
    for c in yag:
        c.start()
    for n in range(8, 16):
        ychunk(n).start()
    for c in yag:
        c.wait_recv()
    mine = pl.ds(pl.multiple_of(row0, 64), 64)
    xag = [same(stat.at[:, mine, :], xs2.at[d], xr2.at[d], xdev[d]) for d in range(3)]
    for c in xag:
        c.start()

    def forward_z(n):
        zchunk(n).wait_recv()
        dchunk(n).start()
        czchunk(n).start()

    def forward_y(n):
        ychunk(n).wait_recv()
        cychunk(n).start()

    def forward_d(n):
        dchunk(n).wait_recv()
        cdchunk(n).start()

    for n in range(5):
        forward_z(n)
        forward_y(n)
    for c in xag:
        c.wait_recv()
    mine = pl.ds(pl.multiple_of(256 * core, 256), 256)
    cag = same(stat.at[:, mine, :], cs2.at[0], cr2.at[0], cpart)
    cag.start()
    for n in range(5, 8):
        forward_z(n)
        forward_y(n)
    cag.wait_recv()
    for c in ownc[4:]:
        c.wait_recv()

    def forward(slot):
        gn = gain[blk * 32 + slot]
        sh = shift[blk * 32 + slot]
        for h in range(0, N, 128):
            rows = slice(h, h + 128)
            v = fld[slot, rows, :].astype(F32)
            nrm = ((v - stat[0, rows, :]) * stat[1, rows, :] * gn + sh).astype(BF)
            a = jnp.dot(nrm, fwd_t[...], preferred_element_type=F32)
            stack[h : h + 128, :] = a.astype(BF)
            stack[N + h : N + h + 128, :] = jnp.concatenate([a[:, 128:], -a[:, :128]], 1).astype(BF)
        m = jnp.dot(both_t[...], stack[...], preferred_element_type=F32)
        mode_re[pl.ds(slot, N, stride=RS), :] = m[:, :128]
        mode_im[pl.ds(slot, N, stride=RS), :] = m[:, 128:]

    def step(t, _):
        @pl.when(t < 2)
        def _():
            for k in range(4):
                forward_y(8 + 4 * t + k)

        forward_z(8 + t)
        for k in range(2):
            forward_d(2 * t + k)

        @pl.when(t == 3)
        def _():
            for n in range(16):
                cychunk(n).wait_recv()

        @pl.when(t == 4)
        def _():
            for n in range(8):
                czchunk(n).wait_recv()

        @pl.when(t == 5)
        def _():
            for n in range(8):
                cdchunk(n).wait_recv()

        @pl.when(t == 6)
        def _():
            for n in range(8, 12):
                czchunk(n).wait_recv()
                cdchunk(n).wait_recv()

        @pl.when(t == 7)
        def _():
            for n in range(12, 16):
                czchunk(n).wait_recv()
                cdchunk(n).wait_recv()

        def one(e, _):
            lo, hi = lax.rem(e, 2), lax.div(e, 2)
            early = t < 4
            late = t > 5
            dy = jnp.where(early, lax.div(t, 2), jnp.where(late, hi, t - 4))
            dz = jnp.where(early, 0, 1)
            dc = jnp.where(early, lax.rem(t, 2), lo)
            i = jnp.where(early, e, jnp.where(late, t - 4, hi))
            forward(base(dy, dz, dc) + i)
            return 0

        lax.fori_loop(0, 4, one, 0)
        return 0

    lax.fori_loop(0, 8, step, 0)

    groups = KB // 4

    def mix(t, _):
        def cols(ref):
            return [
                jnp.concatenate(
                    [
                        ref[pl.ds(pl.multiple_of((t * KB + q * 4 + k) * RS, 8), 32), :]
                        for k in range(4)
                    ],
                    0,
                )
                for q in range(groups)
            ]

        re, im = cols(mode_re), cols(mode_im)
        z = jnp.concatenate(
            [jnp.concatenate([re[q], im[q]], 0) for q in range(groups)], 1
        ).astype(BF)
        hid = jnp.dot(big1[...], z, preferred_element_type=F32)
        hid = jnp.maximum(hid + jnp.concatenate([bcol[...]] * groups, 1), 0.0).astype(BF)
        o = jnp.dot(big2[...], hid, preferred_element_type=F32)
        o = jnp.maximum(o - 0.01, 0.0) + jnp.minimum(o + 0.01, 0.0)
        for q in range(groups):
            for k in range(4):
                at = pl.ds(t * KB + q * 4 + k, 8, stride=SS)
                shr_re[at, :] = o[k * 8 : k * 8 + 8, q * 128 : q * 128 + 128]
                shr_im[at, :] = o[32 + k * 8 : 40 + k * 8, q * 128 : q * 128 + 128]
        return 0

    lax.fori_loop(0, N // KB, mix, 0)

    def backward(c8):
        at = pl.ds(pl.multiple_of(c8 * SS, 8), N)
        sr, si = shr_re[at, :], shr_im[at, :]
        stack[0:N, :] = jnp.concatenate([sr, si], 1).astype(BF)
        stack[N : 2 * N, :] = jnp.concatenate([-si, sr], 1).astype(BF)
        return jnp.dot(both_t[...], stack[...], preferred_element_type=F32).astype(BF)

    def swap(i):
        return remote(back_out.at[i], back_in.at[i], bs.at[i], br.at[i], cpart)

    def give(i, _):
        back_out[i] = backward((1 - core) * 4 + i)
        swap(i).start()
        return 0

    def keep(i, _):
        back_own[i] = backward(core * 4 + i)
        return 0

    def put(i):
        return pltpu.make_async_copy(out_v.at[i], out_hbm.at[i], outs.at[i])

    def finish(i, _):
        swap(i).wait_recv()
        filt = jnp.dot(back_own[i], inv_t[core], preferred_element_type=F32)
        filt = filt + jnp.dot(back_in[i], inv_t[1 - core], preferred_element_type=F32)
        out_v[i] = (fld[own + i].astype(F32) + filt).astype(BF)
        put(i).start()
        return 0

    lax.fori_loop(0, 4, give, 0)
    lax.fori_loop(0, 4, keep, 0)
    lax.fori_loop(0, 4, finish, 0)

    def drain(first, send, to):
        ref = fld.at[pl.ds(first, 4)]
        same(ref, send, zr.at[0], to).wait_send()

    drain(own, zs.at[0], zpart)
    drain(own, ys.at[0], ypart)
    drain(own, os.at[0], cpart)
    drain(base(0, 1, 0), ds.at[0], ypart)
    drain(base(1, 0, 0), cys.at[0], cpart)
    drain(base(0, 1, 0), czs.at[0], cpart)
    drain(base(1, 1, 0), cds.at[0], cpart)
    for c in xrs + yrs + [zex] + yag + xag + [cag]:
        c.wait_send()
    for i in range(4):
        swap(i).wait_send()
        put(i).wait()


def per_device(fields, norm_gain, norm_shift, first_weight, second_weight, first_bias):
    fwd, inv, both = tables()
    dma = pltpu.SemaphoreType.DMA
    vm, sm, hbm = pltpu.VMEM, pltpu.SMEM, pl.ANY
    spec = lambda s: pl.BlockSpec(memory_space=s)
    return pl.pallas_call(
        kernel,
        out_shape=jax.ShapeDtypeStruct((4, N, N), BF),
        in_specs=[spec(s) for s in (hbm, sm, sm, vm, vm, vm, hbm, hbm, hbm)],
        out_specs=spec(hbm),
        scratch_shapes=[
            vm((32, N, N), BF),
            vm((N * RS, 128), F32),
            vm((N * RS, 128), F32),
            vm((8 * SS, 128), F32),
            vm((8 * SS, 128), F32),
            vm((2, N, N), F32),
            vm((2, 256, N), F32),
            vm((3, 2, 64, N), F32),
            vm((2, 64, N), F32),
            vm((3, 2, 16, N), F32),
            vm((2, 16, N), F32),
            vm((2, 16, N), F32),
            vm((N, 256), BF),
            vm((2, 256, N), BF),
            vm((N, 2 * N), BF),
            vm((256, 256), BF),
            vm((64, 256), BF),
            vm((256, 128), F32),
            vm((2 * N, 256), BF),
            vm((4, N, 256), BF),
            vm((4, N, 256), BF),
            vm((4, N, 256), BF),
            vm((4, N, N), BF),
        ]
        + [
            dma((n,))
            for n in (
                1, 16, 1, 16, 1, 16, 1, 8, 1, 16, 1, 16, 1, 16,
                3, 3, 3, 3, 1, 1, 3, 3, 3, 3, 1, 1, 4, 4, 4, 3, 4,
            )
        ],
        compiler_params=pltpu.CompilerParams(
            collective_id=0, has_side_effects=True, vmem_limit_bytes=67043328
        ),
        name="afno",
    )(fields, norm_gain, norm_shift, first_weight, second_weight, first_bias, fwd, inv, both)


def solution(mesh):
    return jax.shard_map(
        per_device,
        mesh=mesh,
        in_specs=(P(("batch", "grid"), None, None), P(), P(), P(), P(), P()),
        out_specs=P(("batch", "grid"), None, None),
        check_vma=False,
    )
```

```python
import functools
import math

import jax
import jax.numpy as jnp
import ml_dtypes
import numpy as np
from jax import lax
from jax.experimental import pallas as pl
from jax.experimental.pallas import tpu as pltpu
from jax.sharding import PartitionSpec as P

MESH = pl.DeviceIdType.MESH
BF = jnp.bfloat16
F32 = jnp.float32
N = 512
ROWS = 128
RS = 40
SS = 520
KB = 64


ZA = 8
YB = 4


def tables():
    half = N // 2
    idx = np.arange(N)
    step = np.float32(2.0 * math.pi / N)
    scale = np.float32(1.0 / math.sqrt(N))
    angle_w = ((idx[:, None] * np.arange(half)[None, :]) % N).astype(np.float32) * step
    cos_w, sin_w = np.cos(angle_w), np.sin(angle_w)
    weight = np.where(np.arange(half) == 0, 1.0, 2.0).astype(np.float32)
    re, im = cos_w * scale, -sin_w * scale
    fwd = np.stack(
        [np.concatenate([re[:, s], im[:, s]], 1) for s in (slice(0, 128), slice(128, 256))]
    )
    ire, iim = (cos_w * weight * scale).T, (-sin_w * weight * scale).T
    inv = np.stack(
        [np.concatenate([ire[s], iim[s]], 0) for s in (slice(0, 128), slice(128, 256))]
    )
    angle_h = ((idx[:, None] * idx[None, :]) % N).astype(np.float32) * step
    both = np.concatenate([np.cos(angle_h) * scale, np.sin(angle_h) * scale], 1)
    cast = lambda a: a.astype(ml_dtypes.bfloat16)
    return cast(fwd), cast(inv), cast(both)


def kernel(
    f_hbm, gain, shift, w1, w2, bias, fwd_hbm, inv_hbm, both_hbm,
    out_hbm,
    fld, mode_re, mode_im, shr_re, shr_im, stat, part, xbuf, xsum, ybuf, ysum, zbuf,
    fwd_t, inv_t, both_t, big1, big2, bcol, stack, back_own, back_out, back_in, out_v,
    zs, zr, ys, yr, ds, dr, os, orr, cys, cyr, czs, czr, cds, cdr,
    xs1, xr1, ys1, yr1, zs1, zr1, ys2, yr2, xs2, xr2, cs2, cr2, bs, br, loc, tab, outs,
):
    b = lax.axis_index("batch")
    g = lax.axis_index("grid")
    core = lax.rem(g, 2)
    zh = lax.rem(lax.div(g, 2), 2)
    y = lax.rem(lax.div(g, 4), 4)
    x = lax.div(g, 16)
    yy = lax.rem(y, 2)
    blk = lax.div(g, 8)

    def dev(x_, y_, z_, c_):
        return (b, ((x_ * 4 + y_) * 2 + z_) * 2 + c_)

    def flip(v, d):
        return v + d - 2 * v * d

    def base(dy, dz, dc):
        return ((flip(yy, dy) * 2 + flip(zh, dz)) * 2 + flip(core, dc)) * 4

    ypart = dev(x, y + 1 - 2 * yy, zh, core)
    zpart = dev(x, y, 1 - zh, core)
    cpart = dev(x, y, zh, 1 - core)
    xpeer = [lax.rem(x + 4 - d, 4) for d in (1, 2, 3)]
    ypeer = [lax.rem(y + 4 - d, 4) for d in (1, 2, 3)]
    xdev = [dev(v, y, zh, core) for v in xpeer]
    ydev = [dev(x, v, zh, core) for v in ypeer]

    def remote(src, dst, send, recv, to):
        return pltpu.make_async_remote_copy(
            src_ref=src, dst_ref=dst, send_sem=send, recv_sem=recv, device_id=to, device_id_type=MESH
        )

    own = base(0, 0, 0)
    tabs = [
        pltpu.make_async_copy(fwd_hbm.at[core], fwd_t, tab.at[0]),
        pltpu.make_async_copy(inv_hbm, inv_t, tab.at[1]),
        pltpu.make_async_copy(both_hbm, both_t, tab.at[2]),
    ]
    fetch = [pltpu.make_async_copy(f_hbm.at[i], fld.at[own + i], loc.at[i]) for i in range(4)]
    for c in fetch:
        c.start()

    barrier = pltpu.get_barrier_semaphore()
    peers = xdev + ydev + [zpart, cpart]
    for p in peers:
        pl.semaphore_signal(barrier, inc=1, device_id=p, device_id_type=MESH)
    pl.semaphore_wait(barrier, len(peers))
    for c in fetch:
        c.wait()
    for c in tabs:
        c.start()

    def piece(first, n):
        row = pl.multiple_of((n % 4) * ROWS, ROWS)
        return fld.at[first + n // 4, pl.ds(row, ROWS), :]

    def half(first, n):
        row = pl.multiple_of((n % 8) * 64, 64)
        return fld.at[first + n // 8, pl.ds(row, 64), :]

    def same(ref, send, recv, to):
        return remote(ref, ref, send, recv, to)

    def zchunk(n):
        return same(half(own, n), zs.at[n], zr.at[n], zpart)

    def ychunk(n):
        return same(half(own, n), ys.at[n], yr.at[n], ypart)

    def dchunk(n):
        return same(piece(base(0, 1, 0), n), ds.at[0], dr.at[n], ypart)

    def cychunk(n):
        return same(piece(base(1, 0, 0), n), cys.at[0], cyr.at[n], cpart)

    def czchunk(n):
        return same(piece(base(0, 1, 0), n), czs.at[0], czr.at[n], cpart)

    def cdchunk(n):
        return same(piece(base(1, 1, 0), n), cds.at[0], cdr.at[n], cpart)

    def owncopy(i, h):
        rows = pl.ds(pl.multiple_of(256 * h, 256), 256)
        return fld.at[own + i, rows, :]

    ownc = [same(owncopy(i, 1 - core), os.at[0], orr.at[i], cpart) for i in range(4)]
    ownc += [same(owncopy(i, core), os.at[0], orr.at[4 + i], cpart) for i in range(4)]
    for c in ownc[:4]:
        c.start()
    def pump(chunk, first, last):
        for n in range(first, last):
            if n > 1:
                chunk(n - 2).wait_send()
            chunk(n).start()

    pump(zchunk, 0, 2)
    pump(ychunk, 0, 2)
    for c in ownc[4:]:
        c.start()

    for c in ownc[:4]:
        c.wait_recv()
    other = base(0, 0, 1)

    def partial_sums(r, _):
        row = pl.multiple_of(256 * core + r * 16, 16)
        s1 = jnp.zeros((16, N), F32)
        s2 = jnp.zeros((16, N), F32)
        for first in (own, other):
            for i in range(4):
                v = fld[first + i, pl.ds(row, 16), :].astype(F32)
                s1 = s1 + v
                s2 = s2 + v * v
        at = pl.ds(pl.multiple_of(r * 16, 16), 16)
        part[0, at, :] = s1
        part[1, at, :] = s2
        return 0

    lax.fori_loop(0, 16, partial_sums, 0)

    xrs = [
        remote(
            part.at[:, pl.ds(pl.multiple_of(64 * xpeer[d], 64), 64), :],
            xbuf.at[d], xs1.at[d], xr1.at[d], xdev[d],
        )
        for d in range(3)
    ]
    for c in xrs:
        c.start()

    for c in tabs:
        c.wait()

    def iota(shape, dim):
        return lax.broadcasted_iota(jnp.int32, shape, dim)

    pick = (iota((256, 32), 0) % 32 == iota((256, 32), 1)).astype(BF)
    nt = (((1,), (1,)), ((), ()))

    def expand(rows, w, sel):
        left = lax.dot_general(sel, w, nt, preferred_element_type=F32).astype(BF)
        return lax.dot_general(left, pick, nt, preferred_element_type=F32)

    def complex_matrix(rows, per, sel, w):
        t0 = expand(rows, w[0, blk], sel)
        t1 = expand(rows, w[1, blk], sel)
        r = iota((rows, 256), 0)
        c = iota((rows, 256), 1)
        rp, cp = r // (4 * per), c // 128
        hit = (r // per) % 4 == (c // 32) % 4
        val = jnp.where(rp == cp, t0, jnp.where(rp == 1, t1, -t1))
        return jnp.where(hit, val, 0.0).astype(BF)

    big1[...] = complex_matrix(256, 32, pick, w1)
    chip = yy * 2 + zh
    pick2 = ((iota((64, 32), 0) % 8) + chip * 8 == iota((64, 32), 1)).astype(BF)
    big2[...] = complex_matrix(64, 8, pick2, w2)
    r = iota((256, 256), 0)
    c = iota((256, 256), 1)
    hit = (r % 32) + blk * 32 == c
    value = jnp.where(r < 128, bias[0:1, :], bias[1:2, :])
    col = jnp.sum(jnp.where(hit, value, 0.0), axis=1, keepdims=True)
    bcol[...] = jnp.broadcast_to(col, (256, 128))

    for n in range(2, ZA):
        pump(ychunk, 2 * n - 2, 2 * n)
        pump(zchunk, n, n + 1)
    for c in xrs:
        c.wait_recv()
    mine = pl.ds(pl.multiple_of(64 * x, 64), 64)
    xsum[...] = part[:, mine, :] + xbuf[0] + xbuf[1] + xbuf[2]
    yrs = [
        remote(
            xsum.at[:, pl.ds(pl.multiple_of(16 * ypeer[d], 16), 16), :],
            ybuf.at[d], ys1.at[d], yr1.at[d], ydev[d],
        )
        for d in range(3)
    ]
    for c in yrs:
        c.start()
    for c in yrs:
        c.wait_send()
    pump(ychunk, 2 * ZA - 2, 2 * ZA)
    pump(zchunk, ZA, ZA + 1)
    for c in yrs:
        c.wait_recv()
    mine = pl.ds(pl.multiple_of(16 * y, 16), 16)
    ysum[...] = xsum[:, mine, :] + ybuf[0] + ybuf[1] + ybuf[2]
    zex = remote(ysum, zbuf, zs1.at[0], zr1.at[0], zpart)
    zex.start()
    pump(ychunk, 2 * ZA, 2 * ZA + YB)
    zex.wait_send()
    pump(zchunk, ZA + 1, ZA + 3)
    zex.wait_recv()
    total = ysum[...] + zbuf[...]
    mean = total[0] * (1.0 / 256.0)
    var = total[1] * (1.0 / 256.0) - mean * mean
    row0 = 256 * core + 64 * x
    mine = pl.ds(pl.multiple_of(row0 + 16 * y, 16), 16)
    stat[0, mine, :] = mean
    stat[1, mine, :] = lax.rsqrt(var + 1e-5)
    yag = [same(stat.at[:, mine, :], ys2.at[d], yr2.at[d], ydev[d]) for d in range(3)]
    for c in yag:
        c.start()
    for c in yag:
        c.wait_send()
    pump(zchunk, ZA + 3, ZA + 4)
    pump(ychunk, 2 * ZA + YB, 2 * ZA + YB + 2)
    for c in yag:
        c.wait_recv()
    mine = pl.ds(pl.multiple_of(row0, 64), 64)
    xag = [same(stat.at[:, mine, :], xs2.at[d], xr2.at[d], xdev[d]) for d in range(3)]
    for c in xag:
        c.start()
    for n in range(ZA + 4, 32):
        zchunk(n).start()
    for n in range(2 * ZA + YB + 2, 32):
        ychunk(n).start()

    def forward_z(n):
        zchunk(2 * n).wait_recv()
        zchunk(2 * n + 1).wait_recv()
        dchunk(n).start()
        czchunk(n).start()

    def forward_y(n):
        ychunk(2 * n).wait_recv()
        ychunk(2 * n + 1).wait_recv()
        cychunk(n).start()

    def forward_d(n):
        dchunk(n).wait_recv()
        cdchunk(n).start()

    for n in range(5):
        forward_z(n)
        forward_y(n)
    for c in xag:
        c.wait_recv()
    mine = pl.ds(pl.multiple_of(256 * core, 256), 256)
    cag = same(stat.at[:, mine, :], cs2.at[0], cr2.at[0], cpart)
    cag.start()
    for n in range(5, 8):
        forward_z(n)
        forward_y(n)
    cag.wait_recv()
    for c in ownc[4:]:
        c.wait_recv()

    def forward(slot):
        gn = gain[blk * 32 + slot]
        sh = shift[blk * 32 + slot]
        for h in range(0, N, 128):
            rows = slice(h, h + 128)
            v = fld[slot, rows, :].astype(F32)
            nrm = ((v - stat[0, rows, :]) * stat[1, rows, :] * gn + sh).astype(BF)
            a = jnp.dot(nrm, fwd_t[...], preferred_element_type=F32)
            stack[h : h + 128, :] = a.astype(BF)
            stack[N + h : N + h + 128, :] = jnp.concatenate([a[:, 128:], -a[:, :128]], 1).astype(BF)
        m = jnp.dot(both_t[...], stack[...], preferred_element_type=F32)
        mode_re[pl.ds(slot, N, stride=RS), :] = m[:, :128]
        mode_im[pl.ds(slot, N, stride=RS), :] = m[:, 128:]

    def step(t, _):
        @pl.when(t < 2)
        def _():
            for k in range(4):
                forward_y(8 + 4 * t + k)

        forward_z(8 + t)
        for k in range(2):
            forward_d(2 * t + k)

        @pl.when(t == 3)
        def _():
            for n in range(16):
                cychunk(n).wait_recv()

        @pl.when(t == 4)
        def _():
            for n in range(8):
                czchunk(n).wait_recv()

        @pl.when(t == 5)
        def _():
            for n in range(8):
                cdchunk(n).wait_recv()

        @pl.when(t == 6)
        def _():
            for n in range(8, 12):
                czchunk(n).wait_recv()
                cdchunk(n).wait_recv()

        @pl.when(t == 7)
        def _():
            for n in range(12, 16):
                czchunk(n).wait_recv()
                cdchunk(n).wait_recv()

        def one(e, _):
            lo, hi = lax.rem(e, 2), lax.div(e, 2)
            early = t < 4
            late = t > 5
            dy = jnp.where(early, lax.div(t, 2), jnp.where(late, hi, t - 4))
            dz = jnp.where(early, 0, 1)
            dc = jnp.where(early, lax.rem(t, 2), lo)
            i = jnp.where(early, e, jnp.where(late, t - 4, hi))
            forward(base(dy, dz, dc) + i)
            return 0

        lax.fori_loop(0, 4, one, 0)
        return 0

    lax.fori_loop(0, 8, step, 0)

    groups = KB // 4

    def mix(t, _):
        def cols(ref):
            return [
                jnp.concatenate(
                    [
                        ref[pl.ds(pl.multiple_of((t * KB + q * 4 + k) * RS, 8), 32), :]
                        for k in range(4)
                    ],
                    0,
                )
                for q in range(groups)
            ]

        re, im = cols(mode_re), cols(mode_im)
        z = jnp.concatenate(
            [jnp.concatenate([re[q], im[q]], 0) for q in range(groups)], 1
        ).astype(BF)
        hid = jnp.dot(big1[...], z, preferred_element_type=F32)
        hid = jnp.maximum(hid + jnp.concatenate([bcol[...]] * groups, 1), 0.0).astype(BF)
        o = jnp.dot(big2[...], hid, preferred_element_type=F32)
        o = jnp.maximum(o - 0.01, 0.0) + jnp.minimum(o + 0.01, 0.0)
        for q in range(groups):
            for k in range(4):
                at = pl.ds(t * KB + q * 4 + k, 8, stride=SS)
                shr_re[at, :] = o[k * 8 : k * 8 + 8, q * 128 : q * 128 + 128]
                shr_im[at, :] = o[32 + k * 8 : 40 + k * 8, q * 128 : q * 128 + 128]
        return 0

    lax.fori_loop(0, N // KB, mix, 0)

    def backward(c8):
        at = pl.ds(pl.multiple_of(c8 * SS, 8), N)
        sr, si = shr_re[at, :], shr_im[at, :]
        stack[0:N, :] = jnp.concatenate([sr, si], 1).astype(BF)
        stack[N : 2 * N, :] = jnp.concatenate([-si, sr], 1).astype(BF)
        return jnp.dot(both_t[...], stack[...], preferred_element_type=F32).astype(BF)

    def swap(i):
        return remote(back_out.at[i], back_in.at[i], bs.at[i], br.at[i], cpart)

    def give(i, _):
        back_out[i] = backward((1 - core) * 4 + i)
        swap(i).start()
        return 0

    def keep(i, _):
        back_own[i] = backward(core * 4 + i)
        return 0

    def put(i):
        return pltpu.make_async_copy(out_v.at[i], out_hbm.at[i], outs.at[i])

    def finish(i, _):
        swap(i).wait_recv()
        filt = jnp.dot(back_own[i], inv_t[core], preferred_element_type=F32)
        filt = filt + jnp.dot(back_in[i], inv_t[1 - core], preferred_element_type=F32)
        out_v[i] = (fld[own + i].astype(F32) + filt).astype(BF)
        put(i).start()
        return 0

    lax.fori_loop(0, 4, give, 0)
    lax.fori_loop(0, 4, keep, 0)
    lax.fori_loop(0, 4, finish, 0)

    def drain(first, send, to):
        ref = fld.at[pl.ds(first, 4)]
        same(ref, send, zr.at[0], to).wait_send()

    for n in range(ZA + 2, 32):
        zchunk(n).wait_send()
    for n in range(2 * ZA + YB, 32):
        ychunk(n).wait_send()
    drain(own, os.at[0], cpart)
    drain(base(0, 1, 0), ds.at[0], ypart)
    drain(base(1, 0, 0), cys.at[0], cpart)
    drain(base(0, 1, 0), czs.at[0], cpart)
    drain(base(1, 1, 0), cds.at[0], cpart)
    for c in xrs + xag + [cag]:
        c.wait_send()
    for i in range(4):
        swap(i).wait_send()
        put(i).wait()


def per_device(fields, norm_gain, norm_shift, first_weight, second_weight, first_bias):
    fwd, inv, both = tables()
    dma = pltpu.SemaphoreType.DMA
    vm, sm, hbm = pltpu.VMEM, pltpu.SMEM, pl.ANY
    spec = lambda s: pl.BlockSpec(memory_space=s)
    return pl.pallas_call(
        kernel,
        out_shape=jax.ShapeDtypeStruct((4, N, N), BF),
        in_specs=[spec(s) for s in (hbm, sm, sm, vm, vm, vm, hbm, hbm, hbm)],
        out_specs=spec(hbm),
        scratch_shapes=[
            vm((32, N, N), BF),
            vm((N * RS, 128), F32),
            vm((N * RS, 128), F32),
            vm((8 * SS, 128), F32),
            vm((8 * SS, 128), F32),
            vm((2, N, N), F32),
            vm((2, 256, N), F32),
            vm((3, 2, 64, N), F32),
            vm((2, 64, N), F32),
            vm((3, 2, 16, N), F32),
            vm((2, 16, N), F32),
            vm((2, 16, N), F32),
            vm((N, 256), BF),
            vm((2, 256, N), BF),
            vm((N, 2 * N), BF),
            vm((256, 256), BF),
            vm((64, 256), BF),
            vm((256, 128), F32),
            vm((2 * N, 256), BF),
            vm((4, N, 256), BF),
            vm((4, N, 256), BF),
            vm((4, N, 256), BF),
            vm((4, N, N), BF),
        ]
        + [
            dma((n,))
            for n in (
                32, 32, 32, 32, 1, 16, 1, 8, 1, 16, 1, 16, 1, 16,
                3, 3, 3, 3, 1, 1, 3, 3, 3, 3, 1, 1, 4, 4, 4, 3, 4,
            )
        ],
        compiler_params=pltpu.CompilerParams(
            collective_id=0, has_side_effects=True, vmem_limit_bytes=67043328
        ),
        name="afno",
    )(fields, norm_gain, norm_shift, first_weight, second_weight, first_bias, fwd, inv, both)


def solution(mesh):
    return jax.shard_map(
        per_device,
        mesh=mesh,
        in_specs=(P(("batch", "grid"), None, None), P(), P(), P(), P(), P()),
        out_specs=P(("batch", "grid"), None, None),
        check_vma=False,
    )
```

```python
import functools
import math

import jax
import jax.numpy as jnp
import ml_dtypes
import numpy as np
from jax import lax
from jax.experimental import pallas as pl
from jax.experimental.pallas import tpu as pltpu
from jax.sharding import PartitionSpec as P

MESH = pl.DeviceIdType.MESH
BF = jnp.bfloat16
F32 = jnp.float32
N = 512
ROWS = 128
SS = 136
KB = 64
BAND = 128
ZA = 9
YB = 4
YA = 2
FZ = 4
YM = (3, 5, 7, 9)


def tables():
    half = N // 2
    idx = np.arange(N)
    step = np.float32(2.0 * math.pi / N)
    scale = np.float32(1.0 / math.sqrt(N))
    angle_w = ((idx[:, None] * np.arange(half)[None, :]) % N).astype(np.float32) * step
    cos_w, sin_w = np.cos(angle_w), np.sin(angle_w)
    weight = np.where(np.arange(half) == 0, 1.0, 2.0).astype(np.float32)
    re, im = cos_w * scale, -sin_w * scale
    fwd = np.stack(
        [np.concatenate([re[:, s], im[:, s]], 1) for s in (slice(0, 128), slice(128, 256))]
    )
    ire, iim = (cos_w * weight * scale).T, (-sin_w * weight * scale).T
    inv = np.stack(
        [np.concatenate([ire[s], iim[s]], 0) for s in (slice(0, 128), slice(128, 256))]
    )
    angle_h = ((idx[:, None] * idx[None, :]) % N).astype(np.float32) * step
    both = np.concatenate([np.cos(angle_h) * scale, np.sin(angle_h) * scale], 1)
    cast = lambda a: a.astype(ml_dtypes.bfloat16)
    return cast(fwd), cast(inv), cast(both)


def kernel(
    f_hbm, gain, shift, w1, w2, bias, fwd_hbm, inv_hbm, both_hbm,
    out_hbm,
    fld, modes, stage, shr_re, shr_im, acc, stat, part, xbuf, xsum, ybuf, ysum, zbuf,
    fwd_t, inv_t, both_t, big1, big2, bcol, stack, back_out, back_in, out_v,
    zs, zr, ys, yr, ds, dr, os, orr, cys, cyr, czs, czr, cds, cdr,
    zms, zmr, yms, ymr, dms, dmr,
    xs1, xr1, ys1, yr1, zs1, zr1, ys2, yr2, xs2, xr2, cs2, cr2, bs, br, loc, tab, outs,
):
    b = lax.axis_index("batch")
    g = lax.axis_index("grid")
    core = lax.rem(g, 2)
    zh = lax.rem(lax.div(g, 2), 2)
    y = lax.rem(lax.div(g, 4), 4)
    x = lax.div(g, 16)
    yy = lax.rem(y, 2)
    blk = lax.div(g, 8)

    def dev(x_, y_, z_, c_):
        return (b, ((x_ * 4 + y_) * 2 + z_) * 2 + c_)

    def flip(v, d):
        return v + d - 2 * v * d

    def chip(dy, dz):
        return flip(yy, dy) * 2 + flip(zh, dz)

    def base(dy, dz, dc):
        return (chip(dy, dz) * 2 + flip(core, dc)) * 4

    ypart = dev(x, y + 1 - 2 * yy, zh, core)
    zpart = dev(x, y, 1 - zh, core)
    cpart = dev(x, y, zh, 1 - core)
    xpeer = [lax.rem(x + 4 - d, 4) for d in (1, 2, 3)]
    ypeer = [lax.rem(y + 4 - d, 4) for d in (1, 2, 3)]
    xdev = [dev(v, y, zh, core) for v in xpeer]
    ydev = [dev(x, v, zh, core) for v in ypeer]

    def remote(src, dst, send, recv, to):
        return pltpu.make_async_remote_copy(
            src_ref=src, dst_ref=dst, send_sem=send, recv_sem=recv, device_id=to, device_id_type=MESH
        )

    own = base(0, 0, 0)
    tabs = [
        pltpu.make_async_copy(fwd_hbm.at[core], fwd_t, tab.at[0]),
        pltpu.make_async_copy(inv_hbm, inv_t, tab.at[1]),
        pltpu.make_async_copy(both_hbm, both_t, tab.at[2]),
    ]
    fetch = [pltpu.make_async_copy(f_hbm.at[i], fld.at[own + i], loc.at[i]) for i in range(4)]
    for c in fetch:
        c.start()

    barrier = pltpu.get_barrier_semaphore()
    peers = xdev + ydev + [zpart, cpart]
    for p in peers:
        pl.semaphore_signal(barrier, inc=1, device_id=p, device_id_type=MESH)
    pl.semaphore_wait(barrier, len(peers))
    for c in fetch:
        c.wait()
    for c in tabs:
        c.start()

    def rows_at(first, n, size):
        per = N // size
        row = pl.multiple_of((n % per) * size, size)
        return fld.at[first + n // per, pl.ds(row, size), :]

    def same(ref, send, recv, to):
        return remote(ref, ref, send, recv, to)

    def zchunk(n):
        return same(rows_at(own, n, 64), zs.at[n], zr.at[n], zpart)

    def ychunk(n):
        return same(rows_at(own, n, 64), ys.at[n], yr.at[n], ypart)

    def dchunk(n):
        return same(rows_at(base(0, 1, 0), n, 128), ds.at[0], dr.at[n], ypart)

    def cychunk(n):
        return same(rows_at(base(1, 0, 0), n, 128), cys.at[0], cyr.at[n], cpart)

    def czchunk(n):
        return same(rows_at(base(0, 1, 0), n, 128), czs.at[0], czr.at[n], cpart)

    def cdchunk(n):
        return same(rows_at(base(1, 1, 0), n, 128), cds.at[0], cdr.at[n], cpart)

    def mode_rows(c, n):
        return modes.at[c, 3, pl.ds(pl.multiple_of(n * 512, 512), 512), :]

    def zmode(n):
        return same(mode_rows(chip(0, 0), n), zms.at[n], zmr.at[n], zpart)

    def ymode(n):
        return same(mode_rows(chip(0, 0), n), yms.at[0], ymr.at[n], ypart)

    def dmode(n):
        return same(mode_rows(chip(0, 1), n), dms.at[0], dmr.at[n], ypart)

    def owncopy(i, h):
        rows = pl.ds(pl.multiple_of(256 * h, 256), 256)
        return fld.at[own + i, rows, :]

    def forward_z(n):
        zchunk(2 * n).wait_recv()
        zchunk(2 * n + 1).wait_recv()
        dchunk(n).start()
        czchunk(n).start()

    def forward_y(n):
        ychunk(2 * n).wait_recv()
        ychunk(2 * n + 1).wait_recv()
        cychunk(n).start()

    def forward_d(n):
        dchunk(n).wait_recv()
        cdchunk(n).start()

    ownc = [same(owncopy(i, 1 - core), os.at[0], orr.at[i], cpart) for i in range(4)]
    ownc += [same(owncopy(i, core), os.at[0], orr.at[4 + i], cpart) for i in range(4)]
    for c in ownc[:4]:
        c.start()

    def pump(chunk, first, last):
        for n in range(first, last):
            if n > 1:
                chunk(n - 2).wait_send()
            chunk(n).start()

    pump(zchunk, 0, 2)
    pump(ychunk, 0, 2)
    for c in ownc[4:]:
        c.start()

    for c in ownc[:4]:
        c.wait_recv()
    other = base(0, 0, 1)

    def partial_sums(r, _):
        row = pl.multiple_of(256 * core + r * 16, 16)
        s1 = jnp.zeros((16, N), F32)
        s2 = jnp.zeros((16, N), F32)
        for first in (own, other):
            for i in range(4):
                v = fld[first + i, pl.ds(row, 16), :].astype(F32)
                s1 = s1 + v
                s2 = s2 + v * v
        at = pl.ds(pl.multiple_of(r * 16, 16), 16)
        part[0, at, :] = s1
        part[1, at, :] = s2
        return 0

    lax.fori_loop(0, 16, partial_sums, 0)

    def part_rows(x_, y_):
        return pl.ds(pl.multiple_of(64 * x_ + 16 * y_, 16), 16)

    yown = ypeer + [y]
    xrs = [
        [
            remote(
                part.at[:, part_rows(xpeer[d], yown[p]), :],
                xbuf.at[d, p], xs1.at[d * 4 + p], xr1.at[d * 4 + p], xdev[d],
            )
            for d in range(3)
        ]
        for p in range(4)
    ]
    for c in sum(xrs, []):
        c.start()

    for c in tabs:
        c.wait()

    def iota(shape, dim):
        return lax.broadcasted_iota(jnp.int32, shape, dim)

    ch = iota((256, 32), 0)
    pick = (ch % 32 == iota((256, 32), 1)).astype(BF)
    ch_in = (ch // 64) * 8 + (ch % 2) * 4 + (ch // 16) % 4
    pick_in = (ch_in == iota((256, 32), 1)).astype(BF)
    nt = (((1,), (1,)), ((), ()))

    def expand(w, sel, cols):
        left = lax.dot_general(sel, w, nt, preferred_element_type=F32).astype(BF)
        return lax.dot_general(left, cols, nt, preferred_element_type=F32)

    def complex_matrix(rows, per, sel, w, cols, cpart_, ck):
        t0 = expand(w[0, blk], sel, cols)
        t1 = expand(w[1, blk], sel, cols)
        r = iota((rows, 256), 0)
        rp = r // (4 * per)
        hit = (r // per) % 4 == ck
        val = jnp.where(rp == cpart_, t0, jnp.where(rp == 1, t1, -t1))
        return jnp.where(hit, val, 0.0).astype(BF)

    c1 = iota((256, 256), 1)
    big1[...] = complex_matrix(256, 32, pick, w1, pick_in, (c1 // 2) % 2, (c1 // 4) % 4)
    pick2 = ((iota((64, 32), 0) % 8) + chip(0, 0) * 8 == iota((64, 32), 1)).astype(BF)
    c2 = iota((64, 256), 1)
    big2[...] = complex_matrix(64, 8, pick2, w2, pick, c2 // 128, (c2 // 32) % 4)
    r = iota((256, 256), 0)
    hit = (r % 32) + blk * 32 == c1
    value = jnp.where(r < 128, bias[0:1, :], bias[1:2, :])
    col = jnp.sum(jnp.where(hit, value, 0.0), axis=1, keepdims=True)
    bcol[...] = jnp.broadcast_to(col, (256, 128))

    def clear(i, _):
        acc[i] = jnp.zeros((N, 256), F32)
        return 0

    lax.fori_loop(0, 8, clear, 0)

    for n in range(2, ZA):
        pump(ychunk, 2 * n - 2, 2 * n)
        pump(zchunk, n, n + 1)
    yrs = [
        remote(xsum.at[p], ybuf.at[p], ys1.at[p], yr1.at[p], ydev[p]) for p in range(3)
    ]
    for p in range(4):
        for c in xrs[p]:
            c.wait_recv()
        xsum[p] = part[:, part_rows(x, yown[p]), :] + xbuf[0, p] + xbuf[1, p] + xbuf[2, p]
        if p < 3:
            yrs[p].start()
    for c in yrs:
        c.wait_send()
    pump(ychunk, 2 * ZA - 2, 2 * ZA + YA)
    pump(zchunk, ZA, ZA + 1)
    for c in yrs:
        c.wait_recv()
    ysum[...] = xsum[3] + ybuf[0] + ybuf[1] + ybuf[2]
    zex = remote(ysum, zbuf, zs1.at[0], zr1.at[0], zpart)
    zex.start()
    pump(ychunk, 2 * ZA + YA, 2 * ZA + YB)
    zex.wait_send()
    pump(zchunk, ZA + 1, ZA + 3)
    zex.wait_recv()
    total = ysum[...] + zbuf[...]
    mean = total[0] * (1.0 / 256.0)
    var = total[1] * (1.0 / 256.0) - mean * mean
    row0 = 256 * core

    def stat_rows(x_, y_):
        return stat.at[:, pl.ds(pl.multiple_of(row0 + 64 * x_ + 16 * y_, 16), 16), :]

    mine = pl.ds(pl.multiple_of(row0 + 64 * x + 16 * y, 16), 16)
    stat[0, mine, :] = mean
    stat[1, mine, :] = lax.rsqrt(var + 1e-5)
    yag = [same(stat_rows(x, y), ys2.at[d], yr2.at[d], ydev[d]) for d in range(3)]
    ygot = [same(stat_rows(x, ypeer[d]), ys2.at[d], yr2.at[2 - d], ydev[d]) for d in range(3)]
    xag = [
        [same(stat_rows(x, yown[p]), xs2.at[d * 4 + p], xr2.at[d * 4 + p], xdev[d]) for d in range(3)]
        for p in range(4)
    ]
    for c in yag + xag[3]:
        c.start()
    for c in yag:
        c.wait_send()
    pump(zchunk, ZA + 3, ZA + 4)
    for p in range(3):
        ygot[p].wait_recv()
        for c in xag[p]:
            c.start()

    def quarter(x_, d):
        rows = stat.at[:, pl.ds(pl.multiple_of(row0 + 64 * x_, 64), 64), :]
        return same(rows, cs2.at[d], cr2.at[d], cpart)

    cag = [quarter(v, d) for d, v in enumerate(xpeer + [x])]
    cag[3].start()
    for n in range(ZA + 4, 24):
        zchunk(n).start()
    for n in range(2 * ZA + YB, 24):
        ychunk(n).start()

    for n in range(7):
        if n < FZ:
            forward_z(n)
        forward_y(n)
    for d in range(3):
        for p in range(4):
            xag[p][2 - d].wait_recv()
        cag[d].start()
    for n in range(FZ, 7):
        forward_z(n)
    for n in range(7, 12):
        forward_y(n)
    for c in cag + ownc[4:]:
        c.wait_recv()

    def forward(slot, at):
        gn = gain[blk * 32 + slot]
        sh = shift[blk * 32 + slot]
        for h in range(0, N, 128):
            rows = slice(h, h + 128)
            v = fld[slot, rows, :].astype(F32)
            nrm = ((v - stat[0, rows, :]) * stat[1, rows, :] * gn + sh).astype(BF)
            a = jnp.dot(nrm, fwd_t[...], preferred_element_type=F32)
            stack[h : h + 128, :] = a.astype(BF)
            stack[N + h : N + h + 128, :] = jnp.concatenate([a[:, 128:], -a[:, :128]], 1).astype(BF)
        m = jnp.dot(both_t[...], stack[...], preferred_element_type=F32)
        stage[pl.ds(at, N, stride=4), :] = m[:, :128]
        stage[pl.ds(at + 2, N, stride=4), :] = m[:, 128:]

    def forward_mode(n):
        zmode(n).wait_recv()
        dmode(n).start()

    def unit(t, _):
        for at, n in ((2, 7), (4, 8), (7, 9), (9, 10), (11, 11)):

            @pl.when(t == at)
            def _(n=n):
                forward_z(n)

        for at, n in zip((10, 11), range(2)):

            @pl.when(t == at)
            def _(n=n):
                zmode(n).start()

        for at, n in zip(YM, range(4)):

            @pl.when(t == at)
            def _(n=n):
                ymode(n).start()

        @pl.when(t == 4)
        def _():
            for n in range(12):
                cychunk(n).wait_recv()

        @pl.when(t == 7)
        def _():
            for n in range(8):
                czchunk(n).wait_recv()

        @pl.when(t == 9)
        def _():
            for n in range(4):
                forward_d(n)
            for n in range(4):
                cdchunk(n).wait_recv()

        @pl.when(t == 10)
        def _():
            for n in range(4, 8):
                forward_d(n)
            for n in range(4, 8):
                cdchunk(n).wait_recv()

        @pl.when(t == 11)
        def _():
            for n in range(8, 12):
                czchunk(n).wait_recv()

        @pl.when(t == 12)
        def _():
            for n in range(8, 12):
                forward_d(n)
            zmode(0).wait_send()
            zmode(2).start()
            for n in range(8, 12):
                cdchunk(n).wait_recv()

        late = t > 10
        diag = t > 8
        dy = jnp.where(late, t - 11, jnp.where(diag, 1, jnp.where(t > 6, 0, jnp.where(t > 3, 1, 0))))
        dz = jnp.where(t > 6, 1, 0)
        i = jnp.where(
            late, 2,
            jnp.where(
                diag, t - 9,
                jnp.where(t > 6, t - 7, jnp.where(t > 3, t - 4, jnp.where(t == 0, 3, t - 1))),
            ),
        )
        c = chip(dy, dz)

        def one(e, _):
            forward(c * 8 + e * 4 + i, e)
            return 0

        lax.fori_loop(0, 2, one, 0)
        modes[c, i] = stage[...].astype(BF)

        return 0

    lax.fori_loop(0, 13, unit, 0)
    forward_mode(0)
    zmode(1).wait_send()
    zmode(3).start()

    groups = KB // 4

    def mix(t, k0):
        cols = []
        for q in range(groups):
            at = pl.ds(pl.multiple_of((k0 + t * KB + q * 4) * 4, 16), 16)
            cols.append(jnp.concatenate([modes[j, i, at, :] for j in range(4) for i in range(4)], 0))
        z = jnp.concatenate(cols, 1)
        hid = jnp.dot(big1[...], z, preferred_element_type=F32)
        hid = jnp.maximum(hid + jnp.concatenate([bcol[...]] * groups, 1), 0.0).astype(BF)
        o = jnp.dot(big2[...], hid, preferred_element_type=F32)
        o = jnp.maximum(o - 0.01, 0.0) + jnp.minimum(o + 0.01, 0.0)
        for q in range(groups):
            for k in range(4):
                at = pl.ds(t * KB + q * 4 + k, 8, stride=SS)
                shr_re[at, :] = o[k * 8 : k * 8 + 8, q * 128 : q * 128 + 128]
                shr_im[at, :] = o[32 + k * 8 : 40 + k * 8, q * 128 : q * 128 + 128]
        return k0

    def band(t, _):
        @pl.when(t < 3)
        def _():
            forward_mode(t + 1)

        ymode(t).wait_recv()
        dmode(t).wait_recv()
        k0 = pl.multiple_of(t * BAND, BAND)
        lax.fori_loop(0, BAND // KB, mix, k0)

        left = jnp.concatenate(
            [both_t[:, pl.ds(k0, BAND)], both_t[:, pl.ds(pl.multiple_of(N + k0, BAND), BAND)]], 1
        )

        def backward(c8, _):
            at = pl.ds(pl.multiple_of(c8 * SS, 8), BAND)
            sr, si = shr_re[at, :], shr_im[at, :]
            right = jnp.concatenate(
                [jnp.concatenate([sr, si], 1), jnp.concatenate([-si, sr], 1)], 0
            ).astype(BF)
            acc[c8] = acc[c8] + jnp.dot(left, right, preferred_element_type=F32)
            return 0

        lax.fori_loop(0, 8, backward, 0, unroll=4)
        return 0

    lax.fori_loop(0, N // BAND, band, 0)

    def swap(i):
        return remote(back_out.at[i], back_in.at[i], bs.at[i], br.at[i], cpart)

    def give(i, _):
        back_out[i] = acc[(1 - core) * 4 + i].astype(BF)
        swap(i).start()
        return 0

    def put(i):
        return pltpu.make_async_copy(out_v.at[i], out_hbm.at[i], outs.at[i])

    def finish(i, _):
        filt = jnp.dot(acc[core * 4 + i].astype(BF), inv_t[core], preferred_element_type=F32)
        swap(i).wait_recv()
        filt = filt + jnp.dot(back_in[i], inv_t[1 - core], preferred_element_type=F32)
        out_v[i] = (fld[own + i].astype(F32) + filt).astype(BF)
        put(i).start()
        return 0

    lax.fori_loop(0, 4, give, 0)
    lax.fori_loop(0, 4, finish, 0)

    for n in range(ZA + 2, 24):
        zchunk(n).wait_send()
    for n in range(2 * ZA + YB - 2, 24):
        ychunk(n).wait_send()

    def drain(ref, send, to):
        same(ref, send, zr.at[0], to).wait_send()

    def raw(first):
        return fld.at[pl.ds(first, 3)]

    drain(fld.at[pl.ds(own, 4)], os.at[0], cpart)
    drain(raw(base(0, 1, 0)), ds.at[0], ypart)
    drain(raw(base(1, 0, 0)), cys.at[0], cpart)
    drain(raw(base(0, 1, 0)), czs.at[0], cpart)
    drain(raw(base(1, 1, 0)), cds.at[0], cpart)
    for n in range(2, 4):
        zmode(n).wait_send()
    drain(modes.at[chip(0, 0), 3], yms.at[0], ypart)
    drain(modes.at[chip(0, 1), 3], dms.at[0], ypart)
    for c in sum(xrs, []) + sum(xag, []) + cag:
        c.wait_send()
    for i in range(4):
        swap(i).wait_send()
        put(i).wait()


def per_device(fields, norm_gain, norm_shift, first_weight, second_weight, first_bias):
    fwd, inv, both = tables()
    dma = pltpu.SemaphoreType.DMA
    vm, sm, hbm = pltpu.VMEM, pltpu.SMEM, pl.ANY
    spec = lambda s: pl.BlockSpec(memory_space=s)
    return pl.pallas_call(
        kernel,
        out_shape=jax.ShapeDtypeStruct((4, N, N), BF),
        in_specs=[spec(s) for s in (hbm, sm, sm, vm, vm, vm, hbm, hbm, hbm)],
        out_specs=spec(hbm),
        scratch_shapes=[
            vm((32, N, N), BF),
            vm((4, 4, 4 * N, 128), BF),
            vm((4 * N, 128), F32),
            vm((8 * SS, 128), F32),
            vm((8 * SS, 128), F32),
            vm((8, N, 256), F32),
            vm((2, N, N), F32),
            vm((2, 256, N), F32),
            vm((3, 4, 2, 16, N), F32),
            vm((4, 2, 16, N), F32),
            vm((3, 2, 16, N), F32),
            vm((2, 16, N), F32),
            vm((2, 16, N), F32),
            vm((N, 256), BF),
            vm((2, 256, N), BF),
            vm((N, 2 * N), BF),
            vm((256, 256), BF),
            vm((64, 256), BF),
            vm((256, 128), F32),
            vm((2 * N, 256), BF),
            vm((4, N, 256), BF),
            vm((4, N, 256), BF),
            vm((4, N, N), BF),
        ]
        + [
            dma((n,))
            for n in (
                24, 24, 24, 24, 1, 12, 1, 8, 1, 12, 1, 12, 1, 12,
                4, 4, 1, 4, 1, 4,
                12, 12, 3, 3, 1, 1, 3, 3, 12, 12, 4, 4, 4, 4, 4, 3, 4,
            )
        ],
        compiler_params=pltpu.CompilerParams(
            collective_id=0, has_side_effects=True, vmem_limit_bytes=67043328
        ),
        name="afno",
    )(fields, norm_gain, norm_shift, first_weight, second_weight, first_bias, fwd, inv, both)


def solution(mesh):
    return jax.shard_map(
        per_device,
        mesh=mesh,
        in_specs=(P(("batch", "grid"), None, None), P(), P(), P(), P(), P()),
        out_specs=P(("batch", "grid"), None, None),
        check_vma=False,
    )
```
